64 devices in a mesh: replica: 4 (over x, y), model: 16 (over z, core).
Axes of the slice: x: 2, y: 2, z: 8, core: 2. Of those that a mesh axis runs over, the one named last changes fastest.
The devices are a block of a 4x4x8 slice.
Arguments:
- x: bfloat16 [128, 18432], P('replica'), parts along dimension 0
- w_query: bfloat16 [18432, 12288], P(None, 'model')
- w_key: bfloat16 [18432, 256], replicated
- w_value: bfloat16 [18432, 256], replicated
- w_out: bfloat16 [12288, 18432], P('model')
- k_cache: bfloat16 [128, 1, 4096, 256], P('replica'), parts along dimension 0
- v_cache: bfloat16 [128, 1, 4096, 256], P('replica'), parts along dimension 0
- lengths: int32 [128], P('replica'), parts along dimension 0
Outputs:
- output 1: bfloat16 [128, 18432], P('replica'), parts along dimension 0
- output 2: bfloat16 [128, 1, 256], P('replica'), parts along dimension 0
- output 3: bfloat16 [128, 1, 256], P('replica'), parts along dimension 0
There are 4 independent parts. The reference program is written for one: setup_inputs(seed, part) draws one part's arguments, and reference() takes and returns one part's arrays. A program takes and returns all parts, laid end to end along the dimension named above; an argument that names none is the same for every part.
All inputs are finite; a program needn't handle non-finite values.
Results may differ from the reference program's by a relative error of at most 0.00389493.
Values are sent between devices in bfloat16 or wider.
A program may use at most 768 MiB of HBM per device.

```python
import jax
import jax.numpy as jnp
from jax import lax

D_MODEL = 18432
NUM_HEADS = 48
KV_HEADS = 1
HEAD_DIM = 256
BATCH_SIZE = 32
CONTEXT_LEN = 4096


def draw_lengths(rng_key):
    key_perm, key_long, key_short = jax.random.split(rng_key, 3)
    perm_rank = jax.random.permutation(key_perm, BATCH_SIZE)
    long_count = max(1, BATCH_SIZE // 16)
    long_len = jax.random.randint(key_long, (BATCH_SIZE,), CONTEXT_LEN // 2, CONTEXT_LEN)
    short_len = jax.random.randint(key_short, (BATCH_SIZE,), 1, 33)
    seq_lens = jnp.where(perm_rank < 2 + long_count, long_len, short_len)
    seq_lens = jnp.where(perm_rank == 1, 1, seq_lens)
    seq_lens = jnp.where(perm_rank == 0, CONTEXT_LEN - 1, seq_lens)
    return seq_lens.astype(jnp.int32)


def setup_inputs(seed: int = 0, part: int = 0) -> dict:
    base_key = jax.random.key(seed)
    key_wq, key_wk, key_wv, key_wo = jax.random.split(base_key, 4)
    part_key = jax.random.fold_in(jax.random.key(seed + 1), part)
    key_x, key_kc, key_vc, key_mean, key_len = jax.random.split(part_key, 5)
    q_width = NUM_HEADS * HEAD_DIM
    kv_width = KV_HEADS * HEAD_DIM
    cache_shape = (BATCH_SIZE, KV_HEADS, CONTEXT_LEN, HEAD_DIM)
    x = jax.random.normal(key_x, (BATCH_SIZE, D_MODEL), jnp.float32).astype(jnp.bfloat16)
    w_query = (jax.random.normal(key_wq, (D_MODEL, q_width), jnp.float32) * D_MODEL ** -0.5).astype(jnp.bfloat16)
    w_key = (jax.random.normal(key_wk, (D_MODEL, kv_width), jnp.float32) * D_MODEL ** -0.5).astype(jnp.bfloat16)
    w_value = (jax.random.normal(key_wv, (D_MODEL, kv_width), jnp.float32) * D_MODEL ** -0.5).astype(jnp.bfloat16)
    w_out = (jax.random.normal(key_wo, (q_width, D_MODEL), jnp.float32) * q_width ** -0.5).astype(jnp.bfloat16)
    k_cache = (1.25 * jax.random.normal(key_kc, cache_shape, jnp.float32)).astype(jnp.bfloat16)
    v_mean = jax.random.normal(key_mean, (BATCH_SIZE, KV_HEADS, 1, HEAD_DIM), jnp.float32)
    v_cache = (jax.random.normal(key_vc, cache_shape, jnp.float32) + v_mean).astype(jnp.bfloat16)
    lengths = draw_lengths(key_len)
    return {"x": x, "w_query": w_query, "w_key": w_key, "w_value": w_value, "w_out": w_out, "k_cache": k_cache, "v_cache": v_cache, "lengths": lengths}


def reference(x, w_query, w_key, w_value, w_out, k_cache, v_cache, lengths):
    group_size = NUM_HEADS // KV_HEADS
    inv_sqrt = HEAD_DIM ** -0.5
    q_all = jnp.dot(x, w_query, preferred_element_type=jnp.float32).astype(jnp.bfloat16)
    k_new = jnp.dot(x, w_key, preferred_element_type=jnp.float32).astype(jnp.bfloat16).reshape(BATCH_SIZE, KV_HEADS, HEAD_DIM)
    v_new = jnp.dot(x, w_value, preferred_element_type=jnp.float32).astype(jnp.bfloat16).reshape(BATCH_SIZE, KV_HEADS, HEAD_DIM)
    q_heads = q_all.reshape(BATCH_SIZE, KV_HEADS, group_size, HEAD_DIM)
    positions = jnp.arange(CONTEXT_LEN)

    def one_sequence(item):
        q_seq, k_rows, v_rows, k_one, v_one, seq_len = item
        q_f32 = q_seq.astype(jnp.float32)
        scores = jnp.einsum("grd,gtd->grt", q_f32, k_rows.astype(jnp.float32)) * inv_sqrt
        score_new = jnp.einsum("grd,gd->gr", q_f32, k_one.astype(jnp.float32)) * inv_sqrt
        in_range = positions[None, None, :] < seq_len
        scores = jnp.where(in_range, scores, -jnp.inf)
        row_max = jnp.maximum(jnp.max(scores, axis=-1), score_new)
        weights = jnp.exp(scores - row_max[:, :, None])
        weight_new = jnp.exp(score_new - row_max)
        norm_sum = jnp.sum(weights, axis=-1) + weight_new
        out_sum = jnp.einsum("grt,gtd->grd", weights.astype(jnp.bfloat16).astype(jnp.float32), v_rows.astype(jnp.float32))
        out_sum = out_sum + weight_new.astype(jnp.bfloat16).astype(jnp.float32)[:, :, None] * v_one.astype(jnp.float32)[:, None, :]
        return (out_sum / norm_sum[:, :, None]).astype(jnp.bfloat16)

    attn_out = lax.map(one_sequence, (q_heads, k_cache, v_cache, k_new, v_new, lengths))
    o_flat = attn_out.reshape(BATCH_SIZE, NUM_HEADS * HEAD_DIM)
    y = (x.astype(jnp.float32) + jnp.dot(o_flat, w_out, preferred_element_type=jnp.float32)).astype(jnp.bfloat16)
    return (y, k_new, v_new)
```

```python
import functools

import jax
import jax.numpy as jnp
from jax import lax
from jax.experimental import pallas as pl
from jax.experimental.pallas import tpu as pltpu
from jax.sharding import PartitionSpec as P

MESH = pl.DeviceIdType.MESH
F32 = jnp.float32
BF16 = jnp.bfloat16
LANES = 128
SUB = 8
ANY = pl.BlockSpec(memory_space=pl.ANY)
VMEM = pl.BlockSpec(memory_space=pltpu.VMEM)
SMEM = pl.BlockSpec(memory_space=pltpu.SMEM)
DMA = pltpu.SemaphoreType.DMA
VMEM_LIMIT = 60 * 1024 * 1024


def qkv_kernel(
    heads, chunk, depth, x_ref, wq_ref, wk_ref, wv_ref, q_ref, kv_ref,
    xbuf, wbuf, kvbuf, acc, xsem, wsem, kvsem, ssem, rsem,
):
    rows, d_model = x_ref.shape
    hd = q_ref.shape[1]
    nchunk = d_model // chunk
    blocks = kv_ref.shape[0]
    per = blocks // 2
    kvchunks = kvbuf.shape[0]
    kvrows = kvbuf.shape[1]
    idx = lax.axis_index("model")
    mine = idx % blocks
    first = idx - mine

    barrier = pltpu.get_barrier_semaphore()
    for o in range(1, blocks):
        pl.semaphore_signal(barrier, inc=1, device_id={"model": first + (mine + o) % blocks}, device_id_type=MESH)

    def x_copy(i):
        cols = pl.ds(i * kvrows, kvrows)
        return pltpu.make_async_copy(x_ref.at[:, cols], xbuf.at[:, cols], xsem.at[i])

    def kv_copy(ref, i):
        cols = pl.ds(pl.multiple_of((mine % per) * LANES, LANES), LANES)
        return pltpu.make_async_copy(ref.at[pl.ds(i * kvrows, kvrows), cols], kvbuf.at[i], kvsem.at[i])

    def w_copy(i):
        return pltpu.make_async_copy(
            wq_ref.at[pl.ds(pl.multiple_of(i * chunk, chunk), chunk), :], wbuf.at[i], wsem.at[i]
        )

    for i in range(kvchunks):
        x_copy(i).start()

        @pl.when(mine < per)
        def _():
            kv_copy(wk_ref, i).start()

        @pl.when(mine >= per)
        def _():
            kv_copy(wv_ref, i).start()

    for i in range(depth):
        w_copy(i).start()

    acc[...] = jnp.zeros_like(acc)
    q_ref[...] = jnp.zeros_like(q_ref)
    kv_sum = jnp.zeros((rows, LANES), F32)
    for i in range(kvchunks):
        x_copy(i).wait()
        kv_copy(wk_ref, i).wait()
        kv_sum = kv_sum + jnp.dot(xbuf[:, pl.ds(i * kvrows, kvrows)], kvbuf[i], preferred_element_type=F32)
    kv_ref[mine] = kv_sum.astype(BF16)

    def step(i, carry):
        w_copy(i).wait()

        @pl.when(i + depth < nchunk)
        def _():
            w_copy(i + depth).start()

        cols = pl.ds(pl.multiple_of(i * chunk, chunk), chunk)
        acc[...] += jnp.dot(xbuf[:, cols], wbuf[i], preferred_element_type=F32)
        return carry

    lax.fori_loop(0, 2, step, 0)

    pl.semaphore_wait(barrier, blocks - 1)

    def exchange(o):
        peer = first + (mine + o) % blocks
        return pltpu.make_async_remote_copy(
            src_ref=kv_ref.at[mine], dst_ref=kv_ref.at[mine], send_sem=ssem.at[o - 1], recv_sem=rsem.at[o - 1],
            device_id={"model": peer}, device_id_type=MESH,
        )

    def arrival(o):
        src = (mine + blocks - o) % blocks
        return pltpu.make_async_remote_copy(
            src_ref=kv_ref.at[src], dst_ref=kv_ref.at[src], send_sem=ssem.at[o - 1], recv_sem=rsem.at[o - 1],
            device_id={"model": first + src}, device_id_type=MESH,
        )

    for o in range(1, blocks):
        exchange(o).start()
    lax.fori_loop(2, nchunk, step, 0)
    for b in range(rows):
        for h in range(heads):
            q_ref[pl.ds(b * SUB + h, 1), :] = acc[pl.ds(b, 1), pl.ds(h * hd, hd)].astype(BF16).astype(F32)
    for o in range(1, blocks):
        arrival(o).wait_recv()
        exchange(o).wait_send()


def qkv(x, w_query, w_key, w_value, head_dim):
    rows, d_model = x.shape
    width = w_query.shape[1]
    heads = width // head_dim
    blocks = 2 * w_key.shape[1] // LANES
    chunk = 1024
    nchunk = d_model // chunk
    depth = min(6, nchunk)
    kvchunks = 4
    return pl.pallas_call(
        functools.partial(qkv_kernel, heads, chunk, depth),
        out_shape=(
            jax.ShapeDtypeStruct((rows * SUB, head_dim), F32),
            jax.ShapeDtypeStruct((blocks, rows, LANES), BF16),
        ),
        in_specs=[ANY] * 4,
        out_specs=(VMEM, VMEM),
        scratch_shapes=[
            pltpu.VMEM((rows, d_model), BF16),
            pltpu.VMEM((nchunk, chunk, width), BF16),
            pltpu.VMEM((kvchunks, d_model // kvchunks, LANES), BF16),
            pltpu.VMEM((rows, width), F32),
            DMA((kvchunks,)),
            DMA((nchunk,)),
            DMA((kvchunks,)),
            DMA((blocks - 1,)),
            DMA((blocks - 1,)),
        ],
        compiler_params=pltpu.CompilerParams(collective_id=0, has_side_effects=True, vmem_limit_bytes=VMEM_LIMIT),
        name="qkv",
    )(x, w_query, w_key, w_value)


def attend_kernel(
    heads, depth, len_ref, q_ref, kv_ref, k_ref, v_ref, o_ref,
    k0, v0, kbuf, vbuf, kvf, m_ref, l_ref, acc, o32, wl_b, wl_j, sem0, ksem, vsem,
):
    rows = o_ref.shape[0]
    hd = q_ref.shape[1]
    slots = k_ref.shape[2]
    t0 = k0.shape[1]
    tb = kbuf.shape[1]
    nbuf = kbuf.shape[0]
    per = kv_ref.shape[0] // 2
    scale = hd ** -0.5

    def first_copies(b):
        return (
            pltpu.make_async_copy(k_ref.at[b, 0, pl.ds(0, t0), :], k0.at[b], sem0.at[0, b]),
            pltpu.make_async_copy(v_ref.at[b, 0, pl.ds(0, t0), :], v0.at[b], sem0.at[1, b]),
        )

    def start_first(b, carry):
        for c in first_copies(b):
            c.start()
        return carry

    lax.fori_loop(0, rows, start_first, 0)

    def list_blocks(b, n):
        extra = jnp.maximum(len_ref[b] - t0 + tb - 1, 0) // tb

        def put(j, n):
            wl_b[n] = b
            wl_j[n] = j
            return n + 1

        return lax.fori_loop(0, extra, put, n)

    total = lax.fori_loop(0, rows, list_blocks, 0)

    def block_copies(i):
        slot = i % nbuf
        b = wl_b[i]
        start = pl.multiple_of(jnp.minimum(t0 + wl_j[i] * tb, slots - tb), t0)
        return (
            pltpu.make_async_copy(k_ref.at[b, 0, pl.ds(start, tb), :], kbuf.at[slot], ksem.at[slot]),
            pltpu.make_async_copy(v_ref.at[b, 0, pl.ds(start, tb), :], vbuf.at[slot], vsem.at[slot]),
        )

    def start_block(i, carry):
        for c in block_copies(i):
            c.start()
        return carry

    lax.fori_loop(0, jnp.minimum(total, depth), start_block, 0)

    kvf[...] = kv_ref[...].astype(F32)
    lane0 = lax.broadcasted_iota(jnp.int32, (SUB, t0), 1)

    def first_block(b):
        for c in first_copies(b):
            c.wait()
        q = q_ref[pl.ds(pl.multiple_of(b * SUB, SUB), SUB), :]
        k_one = jnp.concatenate([kvf[p, pl.ds(b, 1), :] for p in range(per)], axis=1)
        v_one = jnp.concatenate([kvf[per + p, pl.ds(b, 1), :] for p in range(per)], axis=1)
        s_new = jnp.sum(q * k_one, axis=1, keepdims=True) * scale
        s = lax.dot_general(q.astype(BF16), k0[b], (((1,), (1,)), ((), ())), preferred_element_type=F32) * scale
        s = jnp.where(lane0 < len_ref[b], s, -jnp.inf)
        m = jnp.maximum(jnp.max(s, axis=1, keepdims=True), s_new)
        e = jnp.exp(s - m)
        e_new = jnp.exp(s_new - m)
        l = jnp.sum(e, axis=1, keepdims=True) + e_new
        n = jnp.dot(e.astype(BF16), v0[b], preferred_element_type=F32)
        n = n + e_new.astype(BF16).astype(F32) * v_one
        at = pl.ds(pl.multiple_of(b * SUB, SUB), SUB)
        m_ref[at, :] = jnp.broadcast_to(m, (SUB, LANES))
        l_ref[at, :] = jnp.broadcast_to(l, (SUB, LANES))
        acc[at, :] = n

    unroll = 8

    def first_group(g, carry):
        for u in range(unroll):
            first_block(g * unroll + u)
        return carry

    lax.fori_loop(0, rows // unroll, first_group, 0)

    lane = lax.broadcasted_iota(jnp.int32, (SUB, tb), 1)

    def block(i, carry):
        slot = i % nbuf
        b = wl_b[i]
        lo = t0 + wl_j[i] * tb
        start = jnp.minimum(lo, slots - tb)
        for c in block_copies(i):
            c.wait()

        @pl.when(i + depth < total)
        def _():
            start_block(i + depth, 0)

        at = pl.ds(pl.multiple_of(b * SUB, SUB), SUB)
        q = q_ref[at, :].astype(BF16)
        s = lax.dot_general(q, kbuf[slot], (((1,), (1,)), ((), ())), preferred_element_type=F32) * scale
        valid = (lane >= lo - start) & (lane < len_ref[b] - start)
        s = jnp.where(valid, s, -jnp.inf)
        m_old = m_ref[at, :][:, :1]
        m = jnp.maximum(jnp.max(s, axis=1, keepdims=True), m_old)
        e = jnp.exp(s - m)
        fade = jnp.exp(m_old - m)
        l = l_ref[at, :][:, :1] * fade + jnp.sum(e, axis=1, keepdims=True)
        n = acc[at, :] * fade + jnp.dot(e.astype(BF16), vbuf[slot], preferred_element_type=F32)
        m_ref[at, :] = jnp.broadcast_to(m, (SUB, LANES))
        l_ref[at, :] = jnp.broadcast_to(l, (SUB, LANES))
        acc[at, :] = n
        return carry

    lax.fori_loop(0, total, block, 0)

    acc[...] = acc[...] / l_ref[...][:, :1]
    for b in range(rows):
        for h in range(heads):
            o32[pl.ds(b, 1), pl.ds(h * hd, hd)] = acc[pl.ds(b * SUB + h, 1), :]
    o_ref[...] = o32[...].astype(BF16)


def attend(q, kv, k_cache, v_cache, lengths, heads):
    rows = k_cache.shape[0]
    slots, hd = k_cache.shape[2:]
    t0 = 64
    tb = min(1024, slots)
    nbuf = 8
    depth = 6
    most = rows * (-(-slots // tb))
    return pl.pallas_call(
        functools.partial(attend_kernel, heads, depth),
        out_shape=jax.ShapeDtypeStruct((rows, heads * hd), BF16),
        in_specs=[SMEM, VMEM, VMEM, ANY, ANY],
        out_specs=VMEM,
        scratch_shapes=[
            pltpu.VMEM((rows, t0, hd), BF16),
            pltpu.VMEM((rows, t0, hd), BF16),
            pltpu.VMEM((nbuf, tb, hd), BF16),
            pltpu.VMEM((nbuf, tb, hd), BF16),
            pltpu.VMEM(kv.shape, F32),
            pltpu.VMEM((rows * SUB, LANES), F32),
            pltpu.VMEM((rows * SUB, LANES), F32),
            pltpu.VMEM((rows * SUB, hd), F32),
            pltpu.VMEM((rows, heads * hd), F32),
            pltpu.SMEM((most,), jnp.int32),
            pltpu.SMEM((most,), jnp.int32),
            DMA((2, rows)),
            DMA((nbuf,)),
            DMA((nbuf,)),
        ],
        compiler_params=pltpu.CompilerParams(vmem_limit_bytes=VMEM_LIMIT),
        name="attend",
    )(lengths, q, kv, k_cache, v_cache)


def out_kernel(
    n, depth, o_ref, w_ref, x_ref, y_ref,
    wbuf, xbuf, part, prx, rx, wsem, xsem, psend, precv, rsend, rrecv, gsend, grecv, hsend, hrecv,
):
    far = n // 2
    subs, r, w = part.shape[2:]
    idx = lax.axis_index("model")
    z = idx // 2
    c = idx % 2
    d = 2 * c - 1
    ahead = ((z + d + n) % n) * 2 + c
    behind = ((z - d + n) % n) * 2 + c
    partner = z * 2 + 1 - c

    barrier = pltpu.get_barrier_semaphore()
    for peer in (ahead, behind, partner):
        pl.semaphore_signal(barrier, inc=1, device_id={"model": peer}, device_id_type=MESH)

    offsets = [far]
    for k in range(far - 1, 0, -1):
        offsets += [k, -k]
    offsets += [0]

    def col(slab, half):
        return pl.multiple_of(slab * (2 * w) + half * w, LANES)

    def w_copy(i):
        slab = (z + offsets[i] + n) % n
        return pltpu.make_async_copy(w_ref.at[:, pl.ds(col(slab, 0), 2 * w)], wbuf.at[i], wsem.at[i])

    x_copy = pltpu.make_async_copy(x_ref.at[:, pl.ds(col(z, c), w)], xbuf, xsem)

    for i in range(depth):
        w_copy(i).start()
    x_copy.start()

    def remote(src, dst, ssem, rsem, peer):
        return pltpu.make_async_remote_copy(
            src_ref=src, dst_ref=dst, send_sem=ssem, recv_sem=rsem, device_id={"model": peer}, device_id_type=MESH
        )

    def pair_copy(i):
        return remote(part.at[i, 1 - c], prx.at[i], psend.at[i], precv.at[i], partner)

    def compute(i):
        w_copy(i).wait()
        if i + depth < n:
            w_copy(i + depth).start()
        res = jnp.dot(o_ref[...], wbuf[i], preferred_element_type=F32)
        for half in range(2):
            for s in range(subs):
                part[i, half, s] = res[s * r:(s + 1) * r, half * w:(half + 1) * w]
        if i == 0:
            pl.semaphore_wait(barrier, 3)
        pair_copy(i).start()

    def place(long, k):
        if k == far:
            return 0
        base = 1 + 2 * (far - 1 - k)
        return base + (1 - c if long else c)

    def reduce_copy(long, k, s):
        lane = 0 if long else 1
        i = place(long, k)
        return remote(
            part.at[i, c, s], rx.at[lane, k - 1, s], rsend.at[lane, k - 1, s], rrecv.at[lane, k - 1, s],
            ahead if long else behind,
        )

    def reduce_stage(long, k):
        i = place(long, k)
        lane = 0 if long else 1
        first = k == (far if long else far - 1)
        pair_copy(i).wait_recv()
        for s in range(subs):
            if first:
                part[i, c, s] = part[i, c, s] + prx[i, s]
            else:
                reduce_copy(long, k + 1, s).wait_recv()
                part[i, c, s] = part[i, c, s] + prx[i, s] + rx[lane, k, s]
            reduce_copy(long, k, s).start()

    def y_at(slab, half, s):
        return y_ref.at[pl.ds(s * r, r), pl.ds(col(slab, half), w)]

    def slab_of(pos, dd):
        if pos <= far:
            return (z - dd * pos + n) % n
        return (z + dd * (pos - far) + n) % n

    def gather_copy(pos, s):
        long = pos <= far
        hops = pos if long else pos - far
        slab = (z - d * (hops - 1) + n) % n if long else (z + d * (hops - 1) + n) % n
        return remote(
            y_at(slab, c, s), y_at(slab, c, s), gsend.at[pos - 1, s], grecv.at[pos - 1, s], ahead if long else behind
        )

    def arrived(pos, s):
        slab = slab_of(pos, d)
        return remote(y_at(slab, c, s), y_at(slab, c, s), gsend.at[pos - 1, s], grecv.at[pos - 1, s], ahead)

    def share_copy(pos, s):
        slab = slab_of(pos, d)
        return remote(y_at(slab, c, s), y_at(slab, c, s), hsend.at[pos, s], hrecv.at[pos, s], partner)

    def shared(pos, s):
        slab = slab_of(pos, -d)
        return remote(y_at(slab, 1 - c, s), y_at(slab, 1 - c, s), hsend.at[pos, s], hrecv.at[pos, s], partner)

    def finish(s):
        reduce_copy(True, 1, s).wait_recv()
        reduce_copy(False, 1, s).wait_recv()
        total = part[n - 1, c, s] + prx[n - 1, s] + rx[0, 0, s] + rx[1, 0, s]
        y = (xbuf[pl.ds(s * r, r), :].astype(F32) + total).astype(BF16)
        y_ref[pl.ds(s * r, r), pl.ds(col(z, c), w)] = y
        gather_copy(1, s).start()
        gather_copy(far + 1, s).start()
        share_copy(0, s).start()

    def forward(pos, s):
        arrived(pos, s).wait_recv()
        if pos not in (far, n - 1):
            gather_copy(pos + 1, s).start()
        share_copy(pos, s).start()

    after = {1: [(True, far)]}
    if far >= 2:
        after.setdefault(min(3, n - 1), []).append((False, far - 1))
        after.setdefault(min(4, n - 1), []).append((True, far - 1))
        for k in range(far - 2, 0, -1):
            step = min(2 * (far - k) + 2, n - 1)
            after.setdefault(step, []).append((False, k))
            after.setdefault(step, []).append((True, k))
    for i in range(n):
        compute(i)
        for long, k in after.get(i, []):
            reduce_stage(long, k)
    x_copy.wait()
    pair_copy(n - 1).wait_recv()
    for s in range(subs):
        finish(s)
    for hops in range(1, far + 1):
        for s in range(subs):
            forward(hops, s)
            if hops < far:
                forward(far + hops, s)
    for s in range(subs):
        for pos in range(n):
            shared(pos, s).wait_recv()
            share_copy(pos, s).wait_send()
        for pos in range(1, n):
            gather_copy(pos, s).wait_send()
        for k in range(1, far + 1):
            reduce_copy(True, k, s).wait_send()
        for k in range(1, far):
            reduce_copy(False, k, s).wait_send()
    for i in range(n):
        pair_copy(i).wait_send()


def out_project(o, w_out, x, n):
    rows, d_model = x.shape
    inner = o.shape[1]
    w = d_model // (2 * n)
    subs = 2
    r = rows // subs
    far = n // 2
    depth = min(4, n)
    return pl.pallas_call(
        functools.partial(out_kernel, n, depth),
        out_shape=jax.ShapeDtypeStruct((rows, d_model), BF16),
        in_specs=[VMEM, ANY, ANY],
        out_specs=VMEM,
        scratch_shapes=[
            pltpu.VMEM((n, inner, 2 * w), BF16),
            pltpu.VMEM((rows, w), BF16),
            pltpu.VMEM((n, 2, subs, r, w), F32),
            pltpu.VMEM((n, subs, r, w), F32),
            pltpu.VMEM((2, far, subs, r, w), F32),
            DMA((n,)),
            DMA,
            DMA((n,)),
            DMA((n,)),
            DMA((2, far, subs)),
            DMA((2, far, subs)),
            DMA((n - 1, subs)),
            DMA((n - 1, subs)),
            DMA((n, subs)),
            DMA((n, subs)),
        ],
        compiler_params=pltpu.CompilerParams(collective_id=1, has_side_effects=True, vmem_limit_bytes=VMEM_LIMIT),
        name="out",
    )(o, w_out, x)


def solution(mesh):
    n = mesh.shape["model"] // 2

    def local_step(x, w_query, w_key, w_value, w_out, k_cache, v_cache, lengths):
        rows = x.shape[0]
        hd = k_cache.shape[3]
        heads = w_query.shape[1] // hd
        q, kv = qkv(x, w_query, w_key, w_value, hd)
        o = attend(q, kv, k_cache, v_cache, lengths, heads)
        y = out_project(o, w_out, x, n)
        per = kv.shape[0] // 2
        k_new = jnp.concatenate([kv[p] for p in range(per)], axis=1).reshape(rows, 1, hd)
        v_new = jnp.concatenate([kv[per + p] for p in range(per)], axis=1).reshape(rows, 1, hd)
        return y, k_new, v_new

    rows_spec = P("replica")
    return jax.shard_map(
        local_step,
        mesh=mesh,
        in_specs=(P("replica", None), P(None, "model"), P(), P(), P("model", None), rows_spec, rows_spec, rows_spec),
        out_specs=(rows_spec, rows_spec, rows_spec),
        check_vma=False,
    )
```
